32 devices in a mesh: grp: 4 (over y, core), blk: 8 (over z, x).
Axes of the slice: x: 2, y: 2, z: 4, core: 2. Of those that a mesh axis runs over, the one named last changes fastest.
Arguments:
- primal: float32 [262144], P(('blk', 'grp')), may hold values from -3 to 3
- dual: float32 [131072], P(('blk', 'grp')), may hold values from -3 to 3
- objective: float32 [262144], P(('blk', 'grp')), may hold values from -6 to 6
- lower: float32 [262144], P(('blk', 'grp')), may hold values from -2 to -0.5
- upper: float32 [262144], P(('blk', 'grp')), may hold values from 0.5 to 2
- bound_kind: int32 [262144], P(('blk', 'grp')), may hold values from 0 to 3
- rhs: float32 [131072], P(('blk', 'grp')), may hold values from -6 to 6
- row_kind: int32 [131072], P(('blk', 'grp')), may hold values 0 or 1
- q_tiles: float32 [4, 32, 512, 512], P('grp', 'blk'), may hold values from -0.25 to 0.25
- q_index: int32 [4, 2, 32], P('grp', None, 'blk'), may hold values from 0 to 127
- k_tiles: float32 [4, 48, 512, 512], P('grp', 'blk'), may hold values from -0.25 to 0.25
- k_rows: int32 [4, 48], P('grp', 'blk'), may hold values from 0 to 31
- k_cols: int32 [4, 48], P('grp', 'blk'), may hold values from 0 to 127
Outputs:
- final_primal: float32 [262144], P(('blk', 'grp'))
- final_dual: float32 [131072], P(('blk', 'grp'))
- primal_weight: float32 [], replicated
The draws below stay inside these ranges and needn't reach their ends.
Inputs may be any that keep to these rules, and one draw needn't show every extreme that they name: `q_index`: row and column tile indices of Hessian tiles, within the column group. `k_rows`: row tile within the tile's dual block. `bound_kind`: 0 free, 1 lower bound only, 2 both bounds, 3 upper bound only.
All inputs are finite; a program needn't handle non-finite values. No bound on the sum of `row_kind` on one device may be relied on, other than what follows from the above.
Results may differ from the reference program's by a relative error of at most 0.00017.
Values sent between devices are 32-bit elements; how exact they have to be, the bound alone decides.
A program may use at most 64 MiB of HBM per device.

```python
import jax
import jax.numpy as jnp
from jax import lax

TILE = 512
X_DEV = 8192
Y_DEV = 4096
KT = 6
ITERS = 2
NX = 262144
M = 131072
GT_COUNT = 128
RT = 32
QTILES = 32
KTILES = 48
N_GRP = 4
N_BLK = 8


def place_ends(result, rng, smallest, top_value):
    dims = result.shape
    place = [jax.random.randint(jax.random.fold_in(rng, axis), (), 0, dims[axis]) for axis in range(len(dims))]
    result = result.at[tuple(place)].set(smallest)
    longest = dims.index(max(dims))
    place[longest] = (place[longest] + 1) % dims[longest]
    return result.at[tuple(place)].set(top_value)


def steps_of(key, extent, split, low, largest):
    def one(axis_at, blocks):
        draws = jax.random.uniform(jax.random.fold_in(jax.random.fold_in(key, 6), axis_at), (blocks,), jnp.float32, low / len(split), largest / len(split))
        return jnp.repeat(jnp.exp(draws), extent[axis_at] // blocks).reshape((-1,) + (1,) * (len(extent) - axis_at - 1))

    gain = one(*split[0])
    for cut in split[1:]:
        gain = gain * one(*cut)
    return gain


def scatter_about(key, shape, spread, reach, cuts=(), kind=jnp.bfloat16):
    result = spread * jax.random.normal(key, shape, jnp.float32)
    if cuts:
        result = result * steps_of(key, shape, cuts, -0.22, 0.18)
    return jnp.clip(result, -reach, reach).astype(kind)


def setup_inputs(seed: int = 0) -> dict:
    keys = jax.random.split(jax.random.key(seed), 14)
    return {
        "primal": scatter_about(keys[0], (NX,), 0.5, 3.0, ((0, 32),), jnp.float32),
        "dual": scatter_about(keys[1], (M,), 0.5, 3.0, ((0, 32),), jnp.float32),
        "objective": scatter_about(keys[2], (NX,), 1.0, 6.0, ((0, 32),), jnp.float32),
        "lower": jnp.clip(-2.0 + 1.5 * jax.random.uniform(keys[3], (NX,), jnp.float32) ** steps_of(keys[3], (NX,), ((0, 32),), -0.2, 0.2), -2.0, -0.5),
        "upper": jnp.clip(0.5 + 1.5 * jax.random.uniform(keys[4], (NX,), jnp.float32) ** steps_of(keys[4], (NX,), ((0, 32),), -0.2, 0.2), 0.5, 2.0),
        "bound_kind": place_ends(jax.random.randint(keys[5], (NX,), 0, 4), jax.random.fold_in(keys[5], 1), 0, 3).astype(jnp.int32),
        "rhs": scatter_about(keys[6], (M,), 1.0, 6.0, ((0, 32),), jnp.float32),
        "row_kind": place_ends((jax.random.randint(keys[7], (M,), 0, 2) < 1).astype(jnp.int32), jax.random.fold_in(keys[7], 1), 0, 1),
        "q_tiles": scatter_about(keys[8], (N_GRP, QTILES, TILE, TILE), TILE ** -0.5, 0.25, ((0, 4), (1, 8)), jnp.float32),
        "q_index": place_ends(jax.random.randint(keys[9], (N_GRP, 2, QTILES), 0, GT_COUNT), jax.random.fold_in(keys[9], 1), 0, GT_COUNT - 1).astype(jnp.int32),
        "k_tiles": scatter_about(keys[10], (N_GRP, KTILES, TILE, TILE), TILE ** -0.5, 0.25, ((0, 4), (1, 8)), jnp.float32),
        "k_rows": place_ends(jax.random.randint(keys[11], (N_GRP, KTILES), 0, RT), jax.random.fold_in(keys[11], 1), 0, RT - 1).astype(jnp.int32),
        "k_cols": place_ends(jax.random.randint(keys[12], (N_GRP, KTILES), 0, GT_COUNT), jax.random.fold_in(keys[12], 1), 0, GT_COUNT - 1).astype(jnp.int32),
    }


def apply_tiles(tiles, rows, cols, vec, count):
    pieces = vec.reshape(-1, TILE)[cols]
    product = jnp.einsum('tij,tj->ti', tiles, pieces, precision=lax.Precision.HIGHEST)
    return jnp.zeros((count, TILE), product.dtype).at[rows].add(product).reshape(-1)

def apply_transposed(tiles, rows, cols, vec, count):
    pieces = vec.reshape(-1, TILE)[rows]
    product = jnp.einsum('tij,ti->tj', tiles, pieces, precision=lax.Precision.HIGHEST)
    return jnp.zeros((count, TILE), product.dtype).at[cols].add(product).reshape(-1)

def project(values, lower, upper, bound_kind):
    values = jnp.where((bound_kind == 1) | (bound_kind == 2), jnp.maximum(values, lower), values)
    return jnp.where((bound_kind == 2) | (bound_kind == 3), jnp.minimum(values, upper), values)

def reference(primal, dual, objective, lower, upper, bound_kind, rhs, row_kind, q_tiles, q_index, k_tiles, k_rows, k_cols):
    group_tiles = N_BLK * X_DEV // TILE
    block_tiles = N_GRP * Y_DEV // TILE
    owner = (jnp.arange(N_BLK * KT) // KT).astype(jnp.int32)

    def group_vec(values, group):
        return values.reshape(N_BLK, N_GRP, X_DEV)[:, group, :].reshape(-1)

    def to_layout(parts):
        return jnp.stack([p.reshape(N_BLK, X_DEV) for p in parts], axis=1).reshape(-1)

    def forward(values):
        cons_prod = None
        parts = []
        for group in range(N_GRP):
            column_vec = group_vec(values, group)
            parts.append(apply_tiles(q_tiles[group], q_index[group, 0], q_index[group, 1], column_vec, group_tiles))
            term = apply_tiles(k_tiles[group], owner * block_tiles + k_rows[group], k_cols[group], column_vec, N_BLK * block_tiles)
            cons_prod = term if cons_prod is None else cons_prod + term
        return (cons_prod, to_layout(parts))

    def transposed(duals):
        parts = []
        for group in range(N_GRP):
            parts.append(apply_transposed(k_tiles[group], owner * block_tiles + k_rows[group], k_cols[group], duals, group_tiles))
        return to_layout(parts)
    weight = jnp.asarray(1.0, jnp.float32)
    current, duals = (primal, dual)
    cons_prod, hess_prod = forward(current)
    for step in range(ITERS):
        step_primal = 0.5 / weight
        step_dual = 0.5 * weight
        gradient = hess_prod + objective - transposed(duals)
        updated = project(current - step_primal * gradient, lower, upper, bound_kind)
        next_cons, next_hess = forward(updated)
        extrap = 2.0 * next_cons - cons_prod
        dual_new = duals + step_dual * (rhs - extrap)
        dual_new = jnp.where(row_kind == 1, jnp.maximum(dual_new, 0.0), dual_new)
        primal_sq = jnp.sum((updated - current) ** 2)
        dual_sq = jnp.sum((dual_new - duals) ** 2)
        weight = jnp.sqrt(weight * jnp.sqrt((dual_sq + 1e-06) / (primal_sq + 1e-06)))
        current, duals = (updated, dual_new)
        cons_prod, hess_prod = (next_cons, next_hess)
    return (current, duals, weight)
```

```python
import functools

import jax
import jax.numpy as jnp
from jax import lax
from jax.experimental import pallas as pl
from jax.experimental.pallas import tpu as pltpu
from jax.sharding import PartitionSpec as P

ITERS = 2
EPSILON = 1e-06
STEP_SCALE = 0.5
LANES = 128
CHUNK = 512
MESH = pl.DeviceIdType.MESH
F32 = jnp.float32
BF16 = jnp.bfloat16


def split(values):
    high = values.astype(BF16)
    return high, (values - high.astype(F32)).astype(BF16)


def exchange(axis, count, me, source, target, send, recv):
    def copy(k, slot):
        peer = lax.rem(me + k, count)
        return pltpu.make_async_remote_copy(
            src_ref=source,
            dst_ref=target(me if slot else peer),
            send_sem=send.at[k],
            recv_sem=recv.at[me if slot else peer],
            device_id={axis: peer},
            device_id_type=MESH,
        )

    def start(k, carry):
        copy(k, True).start()
        return carry

    def arrive(k, carry):
        copy(k, False).wait_recv()
        return carry

    def leave(k, carry):
        copy(k, True).wait_send()
        return carry

    lax.fori_loop(1, count, start, 0)
    return (
        lambda: lax.fori_loop(1, count, arrive, 0),
        lambda: lax.fori_loop(1, count, leave, 0),
    )


def segment(ids, start, width, rows, quarters):
    place = lax.broadcasted_iota(jnp.int32, (rows, LANES), 0) * LANES
    place = place + lax.broadcasted_iota(jnp.int32, (rows, LANES), 1) - start
    result = jnp.full((rows, LANES), -1, jnp.int32)
    for p, tile_id in enumerate(ids):
        for q in range(quarters):
            result = jnp.where(place == p * quarters + q, tile_id * quarters + q, result)
    return jnp.where((place >= 0) & (place < width), result, 0)


def kernel(
    n_blk,
    n_grp,
    primal,
    dual,
    objective,
    lower,
    upper,
    bound_kind,
    rhs,
    row_kind,
    q_index,
    k_rows,
    k_cols,
    q_tiles,
    k_tiles,
    x_out,
    y_out,
    w_out,
    raw,
    whi,
    wlo,
    xs,
    ys,
    data,
    rows_data,
    ids_x,
    ids_y,
    sel_x,
    sel_y,
    vals_x,
    vals_y,
    fin,
    cons_now,
    hess_now,
    tile_sem,
    blk_send,
    blk_recv,
    grp_send,
    grp_recv,
):
    blk, grp = lax.axis_index("blk"), lax.axis_index("grp")
    nq, nk = q_tiles.shape[0], k_tiles.shape[0]
    tile = q_tiles.shape[-1]
    quarters = tile // LANES
    own_x, own_y = primal.shape[0], dual.shape[0]
    wide_x, wide_y = vals_x.shape[1] // n_blk, vals_y.shape[1] // n_grp
    prod_x, prod_y = (nq + nk) * quarters, nk * quarters

    loads = []
    for t in range(nk + nq):
        source = k_tiles.at[t] if t < nk else q_tiles.at[t - nk]
        loads.append(pltpu.make_async_copy(source, raw.at[t], tile_sem.at[t]))
        loads[-1].start()

    barrier = pltpu.get_barrier_semaphore()

    def greet(axis, count, me):
        def body(k, carry):
            pl.semaphore_signal(
                barrier, inc=1, device_id={axis: lax.rem(me + k, count)}, device_id_type=MESH
            )
            return carry

        lax.fori_loop(1, count, body, 0)

    greet("blk", n_blk, blk)
    greet("grp", n_grp, grp)

    def slot(ref, index, size):
        return ref.at[pl.ds(pl.multiple_of(index * size, size), size)]

    q_rows = [q_index[0, p] for p in range(nq)]
    q_cols = [q_index[1, p] for p in range(nq)]
    c_rows = [k_rows[0, p] for p in range(nk)]
    c_cols = [k_cols[0, p] for p in range(nk)]
    ids_x[blk] = segment(q_rows + c_cols, blk * wide_x, wide_x, ids_x.shape[1], quarters)
    ids_y[grp] = segment(c_rows, grp * wide_y, wide_y, ids_y.shape[1], quarters)
    kind = bound_kind[...]
    mine_x = pl.ds(pl.multiple_of(blk * own_x, own_x), own_x)
    mine_y = pl.ds(pl.multiple_of(grp * own_y, own_y), own_y)
    data[0, mine_x] = objective[...]
    data[1, mine_x] = jnp.where((kind == 1) | (kind == 2), lower[...], -jnp.inf)
    data[2, mine_x] = jnp.where((kind == 2) | (kind == 3), upper[...], jnp.inf)
    rows_data[0, mine_y] = rhs[...]
    rows_data[1, mine_y] = jnp.where(row_kind[...] == 1, 0.0, -jnp.inf)
    xs[mine_x] = primal[...]
    ys[mine_y] = dual[...]

    pl.semaphore_wait(barrier, n_blk + n_grp - 2)

    leaving = []
    used = {"blk": 0, "grp": 0}

    def share(axis, source, target):
        at = used[axis]
        used[axis] += 1
        count, me = (n_blk, blk) if axis == "blk" else (n_grp, grp)
        send, recv = (blk_send, blk_recv) if axis == "blk" else (grp_send, grp_recv)
        arrive, leave = exchange(
            axis, count, me, source, target, send.at[at], recv.at[at]
        )
        leaving.append(leave)
        return arrive

    y_here = share("grp", dual, lambda s: slot(ys, s, own_y))
    x_here = share("blk", primal, lambda s: slot(xs, s, own_x))
    ids_y_here = share("grp", ids_y.at[grp], lambda s: ids_y.at[s])
    ids_x_here = share("blk", ids_x.at[blk], lambda s: ids_x.at[s])

    def planes(ref, index, size):
        return ref.at[:, pl.ds(pl.multiple_of(index * size, size), size)]

    rows_here = share("grp", planes(rows_data, grp, own_y), lambda s: planes(rows_data, s, own_y))
    data_here = share("blk", planes(data, blk, own_x), lambda s: planes(data, s, own_x))

    for t in range(nk + nq):
        loads[t].wait()
        whi[t], wlo[t] = split(raw[t])

    row = lax.broadcasted_iota(jnp.int32, (16, tile), 0)

    def product(vector, index, t, transposed):
        piece = jnp.concatenate(
            [vector[pl.ds(index * quarters + q, 1), :] for q in range(quarters)], axis=1
        )
        high = piece.astype(BF16).astype(F32)
        left = jnp.where(row == 0, high, jnp.where(row == 1, piece - high, 0.0)).astype(BF16)
        dims = (((1,), (0 if transposed else 1,)), ((), ()))
        out = lax.dot_general(left, whi[t], dims, preferred_element_type=F32)
        out = out + lax.dot_general(left, wlo[t], dims, preferred_element_type=F32)
        return out[0:1] + out[1:2]

    def put(ref, first, values):
        for q in range(quarters):
            ref[pl.ds(first + q, 1), :] = values[:, q * LANES : (q + 1) * LANES]

    def send_gradient(step, scalar):
        mine = vals_x.at[step, pl.ds(pl.multiple_of(blk * wide_x, 8), wide_x)]
        for p in range(nk):
            put(mine, (nq + p) * quarters, -product(ys, c_rows[p], p, True))
        if step == 0:
            x_here()
            hessian()
        mine[: nq * quarters] = hess_now[...]
        mine[prod_x:] = jnp.broadcast_to(scalar, (wide_x - prod_x, LANES))
        return share(
            "blk", mine, lambda s: vals_x.at[step, pl.ds(pl.multiple_of(s * wide_x, 8), wide_x)]
        )

    def hessian():
        for p in range(nq):
            put(hess_now, p * quarters, product(xs, q_cols[p], nk + p, False))

    def constraint(step, scalar):
        mine = vals_y.at[step, pl.ds(pl.multiple_of(grp * wide_y, 8), wide_y)]
        for p in range(nk):
            fresh = product(xs, c_cols[p], p, False)
            for q in range(quarters):
                part = fresh[:, q * LANES : (q + 1) * LANES]
                at = pl.ds(p * quarters + q, 1)
                mine[at, :] = 2.0 * part - cons_now[at, :]
                cons_now[at, :] = part
        mine[prod_y:] = jnp.broadcast_to(scalar, (wide_y - prod_y, LANES))
        return share(
            "grp", mine, lambda s: vals_y.at[step, pl.ds(pl.multiple_of(s * wide_y, 8), wide_y)]
        )

    def gathered(selector, values):
        both = jnp.dot(selector, values, preferred_element_type=F32)
        return both[:, :LANES] + both[:, LANES:]

    def scalar_sum(ref, count, wide, at):
        total = ref[pl.ds(at, 1), :]
        for s in range(1, count):
            total = total + ref[pl.ds(s * wide + at, 1), :]
        return total

    def full_sum(values):
        return jnp.sum(jnp.sum(values, axis=0, keepdims=True), axis=1, keepdims=True)

    chunk_x = min(CHUNK, n_blk * own_x)
    chunk_y = min(CHUNK, n_grp * own_y)

    def selectors():
        ids_y_here()
        ids_x_here()
        for ref, ids, chunk in ((sel_y, ids_y, chunk_y), (sel_x, ids_x, chunk_x)):
            codes = jnp.sum(ids[...], axis=0)

            def body(c, carry):
                base = pl.multiple_of(c * chunk, chunk)
                at = lax.broadcasted_iota(jnp.int32, (chunk, LANES), 0) + base
                for k in range(ref.shape[1] // LANES):
                    hit = at == codes[k : k + 1, :]
                    ref[pl.ds(base, chunk), k * LANES : (k + 1) * LANES] = jnp.where(
                        hit, 1.0, 0.0
                    ).astype(BF16)
                return carry

            lax.fori_loop(0, ref.shape[0] // chunk, body, 0)

    def primal_step(step, tau):
        values = jnp.concatenate(split(vals_x[step]), axis=1)

        def body(c, total):
            at = pl.ds(pl.multiple_of(c * chunk_x, chunk_x), chunk_x)
            gradient = gathered(sel_x[at], values) + data[0, at]
            now = xs[at]
            new = jnp.minimum(jnp.maximum(now - tau * gradient, data[1, at]), data[2, at])
            xs[at] = new
            return total + full_sum((new - now) * (new - now))

        return lax.fori_loop(0, n_blk * own_x // chunk_x, body, jnp.zeros((1, 1), F32))

    def dual_step(step, sigma):
        values = jnp.concatenate(split(vals_y[step]), axis=1)

        def body(c, total):
            at = pl.ds(pl.multiple_of(c * chunk_y, chunk_y), chunk_y)
            extrap = gathered(sel_y[at], values)
            now = ys[at]
            new = jnp.maximum(now + sigma * (rows_data[0, at] - extrap), rows_data[1, at])
            ys[at] = new
            return total + full_sum((new - now) * (new - now))

        return lax.fori_loop(0, n_grp * own_y // chunk_y, body, jnp.zeros((1, 1), F32))

    weight = jnp.ones((1, LANES), F32)
    y_here()
    dual_sq = jnp.zeros((1, 1), F32)
    primal_total = None
    for step in range(ITERS):
        gradient_here = send_gradient(step, dual_sq)
        if step == 0:
            for p in range(nk):
                put(cons_now, p * quarters, product(xs, c_cols[p], p, False))
            selectors()
            data_here()
        gradient_here()
        if step > 0:
            dual_total = scalar_sum(vals_x.at[step], n_blk, wide_x, prod_x)
            weight = jnp.sqrt(
                weight * jnp.sqrt((dual_total + EPSILON) / (primal_total + EPSILON))
            )
        primal_sq = primal_step(step, STEP_SCALE / weight)
        constraint_here = constraint(step, primal_sq)
        if step < ITERS - 1:
            hessian()
        if step == 0:
            rows_here()
        constraint_here()
        primal_total = scalar_sum(vals_y.at[step], n_grp, wide_y, prod_y)
        dual_sq = dual_step(step, STEP_SCALE * weight)

    mine = fin.at[pl.ds(pl.multiple_of(blk * 8, 8), 8)]
    mine[...] = jnp.broadcast_to(dual_sq, (8, LANES))
    last_here = share("blk", mine, lambda s: fin.at[pl.ds(pl.multiple_of(s * 8, 8), 8)])
    x_out[...] = xs[mine_x]
    y_out[...] = ys[mine_y]
    last_here()
    dual_total = scalar_sum(fin, n_blk, 8, 0)
    weight = jnp.sqrt(weight * jnp.sqrt((dual_total + EPSILON) / (primal_total + EPSILON)))
    w_out[...] = weight[:, :1]
    for leave in leaving:
        leave()


def up(value, step):
    return -(-value // step) * step


def shards(
    primal,
    dual,
    objective,
    lower,
    upper,
    bound_kind,
    rhs,
    row_kind,
    q_tiles,
    q_index,
    k_tiles,
    k_rows,
    k_cols,
):
    n_blk, n_grp = lax.axis_size("blk"), lax.axis_size("grp")
    nq, nk, tile = q_tiles.shape[1], k_tiles.shape[1], q_tiles.shape[-1]
    quarters = tile // LANES
    own_x, own_y = primal.shape[0] // LANES, dual.shape[0] // LANES
    wide_x = up((nq + nk) * quarters, 8) + 8
    wide_y = up(nk * quarters, 8) + 8
    depth_x, depth_y = n_blk * wide_x, n_grp * wide_y
    vmem = pl.BlockSpec(memory_space=pltpu.VMEM)
    smem = pl.BlockSpec(memory_space=pltpu.SMEM)
    hbm = pl.BlockSpec(memory_space=pl.ANY)

    def lanes(values):
        return values.reshape(-1, LANES)

    x, y, weight = pl.pallas_call(
        functools.partial(kernel, n_blk, n_grp),
        out_shape=(
            jax.ShapeDtypeStruct((own_x, LANES), F32),
            jax.ShapeDtypeStruct((own_y, LANES), F32),
            jax.ShapeDtypeStruct((1, 1), F32),
        ),
        in_specs=[vmem] * 8 + [smem] * 3 + [hbm] * 2,
        out_specs=(vmem, vmem, vmem),
        scratch_shapes=[
            pltpu.VMEM((nk + nq, tile, tile), F32),
            pltpu.VMEM((nk + nq, tile, tile), BF16),
            pltpu.VMEM((nk + nq, tile, tile), BF16),
            pltpu.VMEM((n_blk * own_x, LANES), F32),
            pltpu.VMEM((n_grp * own_y, LANES), F32),
            pltpu.VMEM((3, n_blk * own_x, LANES), F32),
            pltpu.VMEM((2, n_grp * own_y, LANES), F32),
            pltpu.VMEM((n_blk, up(depth_x // LANES, 8), LANES), jnp.int32),
            pltpu.VMEM((n_grp, up(depth_y // LANES, 8), LANES), jnp.int32),
            pltpu.VMEM((n_blk * own_x, depth_x), BF16),
            pltpu.VMEM((n_grp * own_y, depth_y), BF16),
            pltpu.VMEM((ITERS, depth_x, LANES), F32),
            pltpu.VMEM((ITERS, depth_y, LANES), F32),
            pltpu.VMEM((n_blk * 8, LANES), F32),
            pltpu.VMEM((nk * quarters, LANES), F32),
            pltpu.VMEM((nq * quarters, LANES), F32),
            pltpu.SemaphoreType.DMA((nk + nq,)),
            pltpu.SemaphoreType.DMA((ITERS + 4, n_blk)),
            pltpu.SemaphoreType.DMA((ITERS + 4, n_blk)),
            pltpu.SemaphoreType.DMA((ITERS + 3, n_grp)),
            pltpu.SemaphoreType.DMA((ITERS + 3, n_grp)),
        ],
        compiler_params=pltpu.CompilerParams(
            collective_id=0, has_side_effects=True, vmem_limit_bytes=60 * 1024 * 1024
        ),
    )(
        lanes(primal),
        lanes(dual),
        lanes(objective),
        lanes(lower),
        lanes(upper),
        lanes(bound_kind),
        lanes(rhs),
        lanes(row_kind),
        q_index[0],
        k_rows,
        k_cols,
        q_tiles[0],
        k_tiles[0],
    )
    return x.reshape(-1), y.reshape(-1), weight.reshape(())


def solution(mesh):
    vector = P(("blk", "grp"))
    return jax.shard_map(
        shards,
        mesh=mesh,
        in_specs=(vector,) * 8
        + (
            P("grp", "blk", None, None),
            P("grp", None, "blk"),
            P("grp", "blk", None, None),
            P("grp", "blk"),
            P("grp", "blk"),
        ),
        out_specs=(vector, vector, P()),
        check_vma=False,
    )
```

```python
import functools

import jax
import jax.numpy as jnp
from jax import lax
from jax.experimental import pallas as pl
from jax.experimental.pallas import tpu as pltpu
from jax.sharding import PartitionSpec as P

ITERS = 2
EPSILON = 1e-06
STEP_SCALE = 0.5
LANES = 128
CHUNK = 512
MESH = pl.DeviceIdType.MESH
F32 = jnp.float32
BF16 = jnp.bfloat16


def split(values):
    high = values.astype(BF16)
    return high, (values - high.astype(F32)).astype(BF16)


def exchange(axis, count, me, source, target, send, recv):
    def copy(k, slot):
        peer = lax.rem(me + k, count)
        return pltpu.make_async_remote_copy(
            src_ref=source,
            dst_ref=target(me if slot else peer),
            send_sem=send.at[k],
            recv_sem=recv.at[me if slot else peer],
            device_id={axis: peer},
            device_id_type=MESH,
        )

    def start(k, carry):
        copy(k, True).start()
        return carry

    def arrive(k, carry):
        copy(k, False).wait_recv()
        return carry

    def leave(k, carry):
        copy(k, True).wait_send()
        return carry

    lax.fori_loop(1, count, start, 0)
    return (
        lambda: lax.fori_loop(1, count, arrive, 0),
        lambda: lax.fori_loop(1, count, leave, 0),
    )


def segment(ids, start, width, rows, quarters):
    place = lax.broadcasted_iota(jnp.int32, (rows, LANES), 0) * LANES
    place = place + lax.broadcasted_iota(jnp.int32, (rows, LANES), 1) - start
    result = jnp.full((rows, LANES), -1, jnp.int32)
    for p, tile_id in enumerate(ids):
        for q in range(quarters):
            result = jnp.where(place == p * quarters + q, tile_id * quarters + q, result)
    return jnp.where((place >= 0) & (place < width), result, 0)


def kernel(
    n_blk,
    n_grp,
    primal,
    dual,
    objective,
    lower,
    upper,
    bound_kind,
    rhs,
    row_kind,
    q_index,
    k_rows,
    k_cols,
    q_tiles,
    k_tiles,
    x_out,
    y_out,
    w_out,
    raw,
    whi,
    wlo,
    xs,
    ys,
    data,
    rows_data,
    ids_x,
    ids_y,
    sel_h,
    sel_t,
    sel_y,
    vals_h,
    vals_t,
    vals_y,
    sums_x,
    sums_y,
    cons_now,
    tile_sem,
    blk_send,
    blk_recv,
    grp_send,
    grp_recv,
):
    blk, grp = lax.axis_index("blk"), lax.axis_index("grp")
    nq, nk = q_tiles.shape[0], k_tiles.shape[0]
    tile = q_tiles.shape[-1]
    quarters = tile // LANES
    own_x, own_y = primal.shape[0], dual.shape[0]
    wide_h, wide_t = nq * quarters, nk * quarters
    pairs = n_blk // 2
    code_h = sel_h.shape[1] // LANES

    loads = []
    for t in range(nk + nq):
        source = k_tiles.at[t] if t < nk else q_tiles.at[t - nk]
        loads.append(pltpu.make_async_copy(source, raw.at[t], tile_sem.at[t]))
        loads[-1].start()

    barrier = pltpu.get_barrier_semaphore()

    def greet(axis, count, me):
        def body(k, carry):
            pl.semaphore_signal(
                barrier, inc=1, device_id={axis: lax.rem(me + k, count)}, device_id_type=MESH
            )
            return carry

        lax.fori_loop(1, count, body, 0)

    greet("blk", n_blk, blk)
    greet("grp", n_grp, grp)

    def slot(ref, index, size):
        return ref.at[pl.ds(pl.multiple_of(index * size, size), size)]

    q_rows = [q_index[0, p] for p in range(nq)]
    q_cols = [q_index[1, p] for p in range(nq)]
    c_rows = [k_rows[0, p] for p in range(nk)]
    c_cols = [k_cols[0, p] for p in range(nk)]
    code_t = ids_x.shape[1] - code_h
    ids_x[blk, :code_h] = segment(q_rows, blk * wide_h, wide_h, code_h, quarters)
    ids_x[blk, code_h:] = segment(c_cols, blk * wide_t, wide_t, code_t, quarters)
    ids_y[grp] = segment(c_rows, grp * wide_t, wide_t, ids_y.shape[1], quarters)
    kind = bound_kind[...]
    mine_x = pl.ds(pl.multiple_of(blk * own_x, own_x), own_x)
    mine_y = pl.ds(pl.multiple_of(grp * own_y, own_y), own_y)
    data[0, mine_x] = objective[...]
    data[1, mine_x] = jnp.where((kind == 1) | (kind == 2), lower[...], -jnp.inf)
    data[2, mine_x] = jnp.where((kind == 2) | (kind == 3), upper[...], jnp.inf)
    rows_data[0, mine_y] = rhs[...]
    rows_data[1, mine_y] = jnp.where(row_kind[...] == 1, 0.0, -jnp.inf)
    xs[mine_x] = primal[...]
    ys[mine_y] = dual[...]

    pl.semaphore_wait(barrier, n_blk + n_grp - 2)

    leaving = []
    used = {"blk": 0, "grp": 0}

    def share(axis, source, target):
        at = used[axis]
        used[axis] += 1
        count, me = (n_blk, blk) if axis == "blk" else (n_grp, grp)
        send, recv = (blk_send, blk_recv) if axis == "blk" else (grp_send, grp_recv)
        arrive, leave = exchange(
            axis, count, me, source, target, send.at[at], recv.at[at]
        )
        leaving.append(leave)
        return arrive

    y_here = share("grp", dual, lambda s: slot(ys, s, own_y))
    x_here = share("blk", primal, lambda s: slot(xs, s, own_x))

    ids_y_here = share("grp", ids_y.at[grp], lambda s: ids_y.at[s])
    def planes(ref, index, size):
        return ref.at[:, pl.ds(pl.multiple_of(index * size, size), size)]

    rows_here = share("grp", planes(rows_data, grp, own_y), lambda s: planes(rows_data, s, own_y))
    outer, inner = lax.div(blk, 2), lax.rem(blk, 2)

    def passing(at, k, theirs, other):
        there = lax.rem(outer + k, pairs) * 2
        if other:
            sent, got, to = there + inner, there + 1 - inner, outer * 2 + 1 - inner
        else:
            sent, got, to = blk, there + inner, there + inner
        return pltpu.make_async_remote_copy(
            src_ref=planes(data, sent, own_x),
            dst_ref=planes(data, got if theirs else sent, own_x),
            send_sem=blk_send.at[at, k],
            recv_sem=blk_recv.at[at, got if theirs else sent],
            device_id={"blk": to},
            device_id_type=MESH,
        )

    def each(first, call):
        def body(k, carry):
            call(k)
            return carry

        lax.fori_loop(first, pairs, body, 0)

    def reserve():
        used["blk"] += 1
        return used["blk"] - 1

    def unpack(t):
        loads[t].wait()
        whi[t], wlo[t] = split(raw[t])

    row = lax.broadcasted_iota(jnp.int32, (16, tile), 0)

    def product(vector, index, t, transposed):
        piece = jnp.concatenate(
            [vector[pl.ds(index * quarters + q, 1), :] for q in range(quarters)], axis=1
        )
        high = piece.astype(BF16).astype(F32)
        left = jnp.where(row == 0, high, jnp.where(row == 1, piece - high, 0.0)).astype(BF16)
        dims = (((1,), (0 if transposed else 1,)), ((), ()))
        out = lax.dot_general(left, whi[t], dims, preferred_element_type=F32)
        out = out + lax.dot_general(left, wlo[t], dims, preferred_element_type=F32)
        return out[0:1] + out[1:2]

    def put(ref, first, values):
        for q in range(quarters):
            ref[pl.ds(first + q, 1), :] = values[:, q * LANES : (q + 1) * LANES]

    def row_block(ref, step, index, size):
        return ref.at[step, pl.ds(pl.multiple_of(index * size, 8), size)]

    def transposed(step):
        mine = row_block(vals_t, step, blk, wide_t)
        for p in range(nk):
            put(mine, p * quarters, -product(ys, c_rows[p], p, True))
        return share("blk", mine, lambda s: row_block(vals_t, step, s, wide_t))

    def hessian(step):
        mine = row_block(vals_h, step, blk, wide_h)
        for p in range(nq):
            put(mine, p * quarters, product(xs, q_cols[p], nk + p, False))
        return share("blk", mine, lambda s: row_block(vals_h, step, s, wide_h))

    def spread(axis, ref, step, value):
        me = blk if axis == "blk" else grp
        ref[step, me] = jnp.broadcast_to(value, (1, LANES))
        return share(axis, ref.at[step, me], lambda s: ref.at[step, s])

    def constraint(step):
        mine = row_block(vals_y, step, grp, wide_t)
        for p in range(nk):
            fresh = product(xs, c_cols[p], p, False)
            for q in range(quarters):
                part = fresh[:, q * LANES : (q + 1) * LANES]
                at = pl.ds(p * quarters + q, 1)
                mine[at, :] = 2.0 * part - cons_now[at, :]
                cons_now[at, :] = part
        return share("grp", mine, lambda s: row_block(vals_y, step, s, wide_t))

    def parts(values):
        return jnp.concatenate(split(values), axis=1)

    def gathered(*terms):
        both = sum(
            jnp.dot(selector, values, preferred_element_type=F32) for selector, values in terms
        )
        return both[:, :LANES] + both[:, LANES:]

    def scalar_sum(ref, step, count):
        total = ref[step, 0]
        for s in range(1, count):
            total = total + ref[step, s]
        return total

    def full_sum(values):
        return jnp.sum(jnp.sum(values, axis=0, keepdims=True), axis=1, keepdims=True)

    chunk_x = min(CHUNK, n_blk * own_x)
    chunk_y = min(CHUNK, n_grp * own_y)

    def selectors():
        ids_y_here()
        ids_x_here()
        codes_x, codes_y = jnp.sum(ids_x[...], axis=0), jnp.sum(ids_y[...], axis=0)
        for ref, codes, chunk in (
            (sel_h, codes_x[:code_h], chunk_x),
            (sel_t, codes_x[code_h:], chunk_x),
            (sel_y, codes_y, chunk_y),
        ):

            def body(c, carry):
                base = pl.multiple_of(c * chunk, chunk)
                at = lax.broadcasted_iota(jnp.int32, (chunk, LANES), 0) + base
                for k in range(ref.shape[1] // LANES):
                    hit = at == codes[k : k + 1, :]
                    ref[pl.ds(base, chunk), k * LANES : (k + 1) * LANES] = jnp.where(
                        hit, 1.0, 0.0
                    ).astype(BF16)
                return carry

            lax.fori_loop(0, ref.shape[0] // chunk, body, 0)

    def primal_step(step, tau):
        from_h, from_t = parts(vals_h[step]), parts(vals_t[step])

        def body(c, total):
            at = pl.ds(pl.multiple_of(c * chunk_x, chunk_x), chunk_x)
            gradient = gathered(
                (sel_h[at, : n_blk * wide_h], from_h), (sel_t[at, : n_blk * wide_t], from_t)
            )
            gradient = gradient + data[0, at]
            now = xs[at]
            new = jnp.minimum(jnp.maximum(now - tau * gradient, data[1, at]), data[2, at])
            xs[at] = new
            return total + full_sum((new - now) * (new - now))

        return lax.fori_loop(0, n_blk * own_x // chunk_x, body, jnp.zeros((1, 1), F32))

    def dual_step(step, sigma):
        values = parts(vals_y[step])

        def body(c, total):
            at = pl.ds(pl.multiple_of(c * chunk_y, chunk_y), chunk_y)
            extrap = gathered((sel_y[at, : n_grp * wide_t], values))
            now = ys[at]
            new = jnp.maximum(now + sigma * (rows_data[0, at] - extrap), rows_data[1, at])
            ys[at] = new
            return total + full_sum((new - now) * (new - now))

        return lax.fori_loop(0, n_grp * own_y // chunk_y, body, jnp.zeros((1, 1), F32))

    weight = jnp.ones((1, LANES), F32)
    for t in range(nk):
        unpack(t)
    y_here()
    transposed_here = transposed(0)
    ids_x_here = share("blk", ids_x.at[blk], lambda s: ids_x.at[s])
    at_own, at_other = reserve(), reserve()
    passing(at_other, 0, False, True).start()
    each(1, lambda k: passing(at_own, k, False, False).start())
    for t in range(nk, nk + nq):
        unpack(t)
    x_here()
    hessian_here = hessian(0)
    for p in range(nk):
        put(cons_now, p * quarters, product(xs, c_cols[p], p, False))

    def forward(k):
        passing(at_own, k, True, False).wait_recv()
        passing(at_other, k, False, True).start()

    each(1, forward)
    selectors()
    each(0, lambda k: passing(at_other, k, True, True).wait_recv())
    for step in range(ITERS):
        hessian_here()
        transposed_here()
        if step > 0:
            dual_here()
            dual_total = scalar_sum(sums_x, step - 1, n_blk)
            weight = jnp.sqrt(
                weight * jnp.sqrt((dual_total + EPSILON) / (primal_total + EPSILON))
            )
        primal_sq = primal_step(step, STEP_SCALE / weight)
        constraint_here = constraint(step)
        primal_here = spread("grp", sums_y, step, primal_sq)
        if step < ITERS - 1:
            hessian_here = hessian(step + 1)
        if step == 0:
            rows_here()
        constraint_here()
        dual_sq = dual_step(step, STEP_SCALE * weight)
        dual_here = spread("blk", sums_x, step, dual_sq)
        if step < ITERS - 1:
            transposed_here = transposed(step + 1)
        primal_here()
        primal_total = scalar_sum(sums_y, step, n_grp)

    x_out[...] = xs[mine_x]
    y_out[...] = ys[mine_y]
    dual_here()
    dual_total = scalar_sum(sums_x, ITERS - 1, n_blk)
    weight = jnp.sqrt(weight * jnp.sqrt((dual_total + EPSILON) / (primal_total + EPSILON)))
    w_out[...] = weight[:, :1]
    each(0, lambda k: passing(at_other, k, False, True).wait_send())
    each(1, lambda k: passing(at_own, k, False, False).wait_send())
    for leave in leaving:
        leave()


def up(value, step):
    return -(-value // step) * step


def shards(
    primal,
    dual,
    objective,
    lower,
    upper,
    bound_kind,
    rhs,
    row_kind,
    q_tiles,
    q_index,
    k_tiles,
    k_rows,
    k_cols,
):
    n_blk, n_grp = lax.axis_size("blk"), lax.axis_size("grp")
    nq, nk, tile = q_tiles.shape[1], k_tiles.shape[1], q_tiles.shape[-1]
    quarters = tile // LANES
    own_x, own_y = primal.shape[0] // LANES, dual.shape[0] // LANES
    wide_h, wide_t = nq * quarters, nk * quarters
    code_h, code_t = up(n_blk * wide_h, LANES), up(n_blk * wide_t, LANES)
    code_y = up(n_grp * wide_t, LANES)
    vmem = pl.BlockSpec(memory_space=pltpu.VMEM)
    smem = pl.BlockSpec(memory_space=pltpu.SMEM)
    hbm = pl.BlockSpec(memory_space=pl.ANY)

    def lanes(values):
        return values.reshape(-1, LANES)

    x, y, weight = pl.pallas_call(
        functools.partial(kernel, n_blk, n_grp),
        out_shape=(
            jax.ShapeDtypeStruct((own_x, LANES), F32),
            jax.ShapeDtypeStruct((own_y, LANES), F32),
            jax.ShapeDtypeStruct((1, 1), F32),
        ),
        in_specs=[vmem] * 8 + [smem] * 3 + [hbm] * 2,
        out_specs=(vmem, vmem, vmem),
        scratch_shapes=[
            pltpu.VMEM((nk + nq, tile, tile), F32),
            pltpu.VMEM((nk + nq, tile, tile), BF16),
            pltpu.VMEM((nk + nq, tile, tile), BF16),
            pltpu.VMEM((n_blk * own_x, LANES), F32),
            pltpu.VMEM((n_grp * own_y, LANES), F32),
            pltpu.VMEM((3, n_blk * own_x, LANES), F32),
            pltpu.VMEM((2, n_grp * own_y, LANES), F32),
            pltpu.VMEM((n_blk, (code_h + code_t) // LANES, LANES), jnp.int32),
            pltpu.VMEM((n_grp, code_y // LANES, LANES), jnp.int32),
            pltpu.VMEM((n_blk * own_x, code_h), BF16),
            pltpu.VMEM((n_blk * own_x, code_t), BF16),
            pltpu.VMEM((n_grp * own_y, code_y), BF16),
            pltpu.VMEM((ITERS, n_blk * wide_h, LANES), F32),
            pltpu.VMEM((ITERS, n_blk * wide_t, LANES), F32),
            pltpu.VMEM((ITERS, n_grp * wide_t, LANES), F32),
            pltpu.VMEM((ITERS, n_blk, 1, LANES), F32),
            pltpu.VMEM((ITERS, n_grp, 1, LANES), F32),
            pltpu.VMEM((nk * quarters, LANES), F32),
            pltpu.SemaphoreType.DMA((nk + nq,)),
            pltpu.SemaphoreType.DMA((3 * ITERS + 4, n_blk)),
            pltpu.SemaphoreType.DMA((3 * ITERS + 4, n_blk)),
            pltpu.SemaphoreType.DMA((2 * ITERS + 3, n_grp)),
            pltpu.SemaphoreType.DMA((2 * ITERS + 3, n_grp)),
        ],
        compiler_params=pltpu.CompilerParams(
            collective_id=0, has_side_effects=True, vmem_limit_bytes=60 * 1024 * 1024
        ),
    )(
        lanes(primal),
        lanes(dual),
        lanes(objective),
        lanes(lower),
        lanes(upper),
        lanes(bound_kind),
        lanes(rhs),
        lanes(row_kind),
        q_index[0],
        k_rows,
        k_cols,
        q_tiles[0],
        k_tiles[0],
    )
    return x.reshape(-1), y.reshape(-1), weight.reshape(())


def solution(mesh):
    vector = P(("blk", "grp"))
    return jax.shard_map(
        shards,
        mesh=mesh,
        in_specs=(vector,) * 8
        + (
            P("grp", "blk", None, None),
            P("grp", None, "blk"),
            P("grp", "blk", None, None),
            P("grp", "blk"),
            P("grp", "blk"),
        ),
        out_specs=(vector, vector, P()),
        check_vma=False,
    )
```
